32 devices in a mesh: batch: 2 (over x), col: 4 (over z), row: 4 (over y, core).
Axes of the slice: x: 2, y: 2, z: 4, core: 2. Of those that a mesh axis runs over, the one named last changes fastest.
Arguments:
- z_one: bfloat16 [2048, 1024, 64], P(('batch', 'row'), 'col'), parts along dimension 0
- z_two: bfloat16 [2048, 1024, 64], P(('batch', 'row'), 'col'), parts along dimension 0
- mask_one: int32 [2048, 1024], P(('batch', 'row'), 'col'), parts along dimension 0
- mask_two: int32 [2048, 1024], P(('batch', 'row'), 'col'), parts along dimension 0
- ln_in_scale: bfloat16 [64], replicated
- w_a: bfloat16 [64, 64], replicated
- w_a_gate: bfloat16 [64, 64], replicated
- w_b: bfloat16 [64, 64], replicated
- w_b_gate: bfloat16 [64, 64], replicated
- w_gate: bfloat16 [64, 64], replicated
- w_out: bfloat16 [64, 64], replicated
- ln_out_scale: bfloat16 [64], replicated
Outputs:
- output 1: bfloat16 [2048, 1024, 64], P(('batch', 'row'), 'col'), parts along dimension 0
- output 2: bfloat16 [2048, 1024, 64], P(('batch', 'row'), 'col'), parts along dimension 0
There are 2 independent parts. The reference program is written for one: setup_inputs(seed, part) draws one part's arguments, and reference() takes and returns one part's arrays. A program takes and returns all parts, laid end to end along the dimension named above; an argument that names none is the same for every part.
All inputs are finite; a program needn't handle non-finite values.
Results may differ from the reference program's by a relative error of at most 0.001.
Values are sent between devices in bfloat16 or wider.
A program may use at most 1 GiB of HBM per device.

```python
import jax
import jax.numpy as jnp
from jax import lax

NRES = 1024
CZ = 64
CHID = 64
ROW_BLOCK = 256


def layer_norm(values, scale):
    row_mean = jnp.mean(values, axis=-1, keepdims=True)
    centered = values - row_mean
    variance = jnp.mean(centered * centered, axis=-1, keepdims=True)
    return centered * lax.rsqrt(variance + 1e-5) * scale.astype(jnp.float32)


def linear(normed, weight):
    flat = normed.reshape(-1, normed.shape[-1])
    result = jnp.dot(flat, weight, preferred_element_type=jnp.float32)
    return result.reshape(normed.shape[:-1] + (weight.shape[1],))


def one_crop(pair, mask, ln_in_scale, w_a, w_a_gate, w_b, w_b_gate, w_gate, w_out, ln_out_scale):
    block_count = NRES // ROW_BLOCK
    pair_blocks = pair.reshape(block_count, ROW_BLOCK, NRES, CZ)
    mask_blocks = mask.reshape(block_count, ROW_BLOCK, NRES)

    def project(block):
        pair_blk, mask_blk = block
        normed = layer_norm(pair_blk.astype(jnp.float32), ln_in_scale).astype(jnp.bfloat16)
        mask_val = mask_blk.astype(jnp.float32)[:, :, None]
        left = mask_val * jax.nn.sigmoid(linear(normed, w_a_gate)) * linear(normed, w_a)
        right = mask_val * jax.nn.sigmoid(linear(normed, w_b_gate)) * linear(normed, w_b)
        return left.astype(jnp.bfloat16), right.astype(jnp.bfloat16)

    left_all, right_all = lax.map(project, (pair_blocks, mask_blocks))
    right_major = jnp.transpose(right_all.reshape(NRES, NRES, CHID).astype(jnp.float32), (2, 0, 1))

    def finish(block):
        pair_blk, left_blk = block
        normed = layer_norm(pair_blk.astype(jnp.float32), ln_in_scale).astype(jnp.bfloat16)
        gate = jax.nn.sigmoid(linear(normed, w_gate))
        left_major = jnp.transpose(left_blk.astype(jnp.float32), (2, 0, 1))
        contracted = jnp.einsum('cik,cjk->ijc', left_major, right_major)
        normed_out = layer_norm(contracted, ln_out_scale).astype(jnp.bfloat16)
        update = linear(normed_out, w_out)
        return (pair_blk.astype(jnp.float32) + gate * update).astype(jnp.bfloat16)

    out_blocks = lax.map(finish, (pair_blocks, left_all))
    return out_blocks.reshape(NRES, NRES, CZ)


def setup_inputs(seed: int = 0, part: int = 0) -> dict:
    root = jax.random.key(seed)
    shared_key, crop_base = jax.random.split(root)
    crop_keys = jax.random.split(jax.random.fold_in(crop_base, part), 4)
    weight_keys = jax.random.split(shared_key, 8)

    def pair_draw(key_in):
        return jax.random.normal(key_in, (NRES, NRES, CZ), jnp.float32).astype(jnp.bfloat16)

    def mask_draw(key_in):
        valid = (jax.random.randint(key_in, (NRES,), 0, 10) != 0).astype(jnp.int32)
        return valid[:, None] * valid[None, :]

    def weight_draw(key_in, fan_in, fan_out):
        values = jax.random.normal(key_in, (fan_in, fan_out), jnp.float32) * fan_in ** -0.5
        return values.astype(jnp.bfloat16)

    def scale_draw(key_in, width):
        return jax.random.uniform(key_in, (width,), jnp.float32, 0.5, 1.5).astype(jnp.bfloat16)

    return {
        'z_one': pair_draw(crop_keys[0]),
        'z_two': pair_draw(crop_keys[1]),
        'mask_one': mask_draw(crop_keys[2]),
        'mask_two': mask_draw(crop_keys[3]),
        'ln_in_scale': scale_draw(weight_keys[0], CZ),
        'w_a': weight_draw(weight_keys[1], CZ, CHID),
        'w_a_gate': weight_draw(weight_keys[2], CZ, CHID),
        'w_b': weight_draw(weight_keys[3], CZ, CHID),
        'w_b_gate': weight_draw(weight_keys[4], CZ, CHID),
        'w_gate': weight_draw(weight_keys[5], CZ, CZ),
        'w_out': weight_draw(weight_keys[6], CHID, CZ),
        'ln_out_scale': scale_draw(weight_keys[7], CHID),
    }


def reference(z_one, z_two, mask_one, mask_two, ln_in_scale, w_a, w_a_gate, w_b, w_b_gate, w_gate, w_out, ln_out_scale):
    out_one = one_crop(z_one, mask_one, ln_in_scale, w_a, w_a_gate, w_b, w_b_gate, w_gate, w_out, ln_out_scale)
    out_two = one_crop(z_two, mask_two, ln_in_scale, w_a, w_a_gate, w_b, w_b_gate, w_gate, w_out, ln_out_scale)
    return (out_one, out_two)
```

```python
import functools

import jax
import jax.numpy as jnp
from jax import lax
from jax.experimental import pallas as pl
from jax.experimental.pallas import tpu as pltpu
from jax.sharding import PartitionSpec as P

MESH = pl.DeviceIdType.MESH
F32 = jnp.float32
BF16 = jnp.bfloat16
G8 = 8


def norm_kernel(z0, z1, m0, m1, s, out):
    scale = s[...]
    for crop, (z, m) in enumerate(((z0, m0), (z1, m1))):
        v = z[...].astype(F32)
        v = v - jnp.mean(v, axis=1, keepdims=True)
        var = jnp.mean(v * v, axis=1, keepdims=True)
        x = (v * lax.rsqrt(var + 1e-5) * scale).astype(BF16)
        mask = m[...].astype(F32)[:, None, :]
        out[crop, 0] = (x.astype(F32) * mask).astype(BF16)


def finish_kernel(z, on, s, wg, wo, out):
    scale = s[...]
    for g in range(z.shape[0] // G8):
        rows = slice(g * G8, (g + 1) * G8)
        zf = z[rows].astype(F32)
        v = zf - jnp.mean(zf, axis=1, keepdims=True)
        var = jnp.mean(v * v, axis=1, keepdims=True)
        x = (v * lax.rsqrt(var + 1e-5) * scale).astype(BF16)
        k = x.shape[1] * G8
        gate = jnp.dot(wg[...], x.reshape(k, x.shape[2]), preferred_element_type=F32)
        half = jnp.dot(wo[...], on[0, g], preferred_element_type=F32)
        upd = ((1.0 + jnp.tanh(gate)) * half).reshape(zf.shape)
        out[rows] = (zf + upd).astype(BF16)


def tri_kernel(nch, ch, gx_in, wa, wb, so, on, gx, rx, A, B, O, xa, xb, st,
               g_sem, r_sem, s_in, s_out, s_f, s_r1, s_r2, l_sem, o_sem):
    del gx_in
    z = lax.axis_index("col")
    r = lax.axis_index("row")
    h = z // 2
    zz = z + h * (3 - 2 * z)
    q = r + h * (3 - 2 * r)
    inner = z + 1 - 2 * h
    outer = 3 * h
    partner = r + 1 - 2 * (r % 2)
    cross = 2 - h
    mid = zz == 1
    end = zz == 0
    owner = q == zz
    relay = q == 2
    n_i, n_k = gx.shape[2], gx.shape[4]
    cr = n_i // nch

    def rows(j):
        return pl.ds(pl.multiple_of(j * cr, cr), cr)

    def gs(c, t, j):
        return gx.at[c, t, rows(j)]

    def rs(c, t, j):
        return rx.at[c, t, rows(j)]

    def cp(src, dst, ssem, rsem, col, row):
        return pltpu.make_async_remote_copy(src_ref=src, dst_ref=dst, send_sem=ssem, recv_sem=rsem,
                                            device_id={"col": col, "row": row}, device_id_type=MESH)

    def p_in(c, j):
        return cp(gs(c, 0, j), gs(c, 1 + zz, j), s_in.at[c, j], g_sem.at[c, zz, j], inner, r)

    def p_out(c, j):
        return cp(gs(c, 0, j), gs(c, 1, j), s_out.at[c, j], g_sem.at[c, 0, j], outer, r)

    def fwd(n, c, j):
        src, dst, col = ((1, 3, inner), (2, 2, outer), (3, 3, outer))[n]
        return cp(gs(c, src, j), gs(c, dst, j), s_f.at[c, n, j], g_sem.at[c, dst - 1, j], col, r)

    def wait_g(c, t, j):
        cp(gs(c, t, j), gs(c, t, j), s_in.at[c, j], g_sem.at[c, t - 1, j], z, r).wait_recv()

    def rx_p(c, t, j):
        return cp(gs(c, t, j), rs(c, t, j), s_r1.at[c, t, j], r_sem.at[c, t, j], z, partner)

    def rx_c(c, t, j):
        return cp(gs(c, t, j), rs(c, t, j), s_r2.at[c, t, j], r_sem.at[c, t, j], z, cross)

    def rx_f(c, t, j):
        return cp(rs(c, t, j), rs(c, t, j), s_r1.at[c, t, j], r_sem.at[c, t, j], z, partner)

    def rx_send(c, t, j):
        rx_c(c, t, j).start()
        rx_p(c, t, j).start()

    @pl.loop(0, nch)
    def _(j):
        p_in(0, j).start()

        @pl.when(mid)
        def _():
            p_out(0, j).start()

        @pl.when(end)
        def _():
            p_in(1, j).start()

    def comm(c, t, j):
        @pl.when((c == 0) & (t == 0) & owner)
        def _():
            rx_send(0, 0, j)

        @pl.when((c == 0) & (t == 2) & owner)
        def _():
            rx_send(1, 0, j)

        @pl.when((c == 0) & (t == 2) & mid)
        def _():
            p_in(1, j).start()

        @pl.when((t == 1) & mid)
        def _():
            wait_g(c, 1, j)
            fwd(0, c, j).start()
            wait_g(c, 2, j)
            fwd(1, c, j).start()

            @pl.when(owner)
            def _():
                rx_send(c, 1, j)
                rx_send(c, 2, j)

        @pl.when((t == 3) & mid)
        def _():
            wait_g(c, 3, j)
            fwd(2, c, j).start()

            @pl.when(owner)
            def _():
                rx_send(c, 3, j)

            @pl.when(c == 0)
            def _():
                p_out(1, j).start()

        @pl.when((t > 0) & end)
        def _():
            for tt in (1, 2, 3):
                @pl.when(t == tt)
                def _():
                    wait_g(c, tt, j)

            @pl.when(owner)
            def _():
                rx_send(c, t, j)

    half = wa.shape[1] // 2

    def project(src, w, dst, j):
        @pl.loop(0, cr // 16)
        def _(s):
            xs = src[pl.ds(pl.multiple_of(s * 16, 16), 16)]
            x0 = xs[:G8].reshape(G8 * ch, n_k)
            x1 = xs[G8:].reshape(G8 * ch, n_k)
            i0 = pl.multiple_of(j * cr + s * 16, 16)
            nc = half // G8
            for p in range(w.shape[0]):
                parts = []
                for xg in (x0, x1):
                    res = jnp.dot(w[p], xg, preferred_element_type=F32)
                    val = res[:half] * (1.0 + jnp.tanh(res[half:]))
                    parts.append(val.reshape(nc, G8, n_k))
                dst[p * nc:(p + 1) * nc, pl.ds(i0, 16), :] = jnp.concatenate(parts, axis=1).astype(BF16)

    @pl.loop(0, 2)
    def _(c):
        @pl.loop(0, ch)
        def _(k):
            O[k] = jnp.zeros(O.shape[1:], F32)

        @pl.loop(0, 4)
        def _(t):
            @pl.loop(0, nch)
            def _(j):
                comm(c, t, j)
                la = pltpu.make_async_copy(gs(c, t, j), xa, l_sem.at[0])
                la.start()

                @pl.when(owner)
                def _():
                    pltpu.make_async_copy(gs(c, t, j), xb, l_sem.at[1]).start()

                la.wait()
                project(xa, wa, A, j)

                @pl.when(jnp.logical_not(owner))
                def _():
                    rx_p(c, t, j).wait_recv()

                    @pl.when(relay)
                    def _():
                        rx_f(c, t, j).start()

                    pltpu.make_async_copy(rs(c, t, j), xb, l_sem.at[1]).start()

                pltpu.make_async_copy(rs(c, t, j), xb, l_sem.at[1]).wait()
                project(xb, wb, B, j)

            @pl.loop(0, ch)
            def _(k):
                O[k] += lax.dot_general(A[k], B[k], (((1,), (1,)), ((), ())), preferred_element_type=F32)

        n_g = n_i // G8
        per = st.shape[1]

        def put(c, b):
            return pltpu.make_async_copy(st.at[b % 2], on.at[c, pl.ds(b * per, per)], o_sem.at[b % 2])

        @pl.loop(0, n_g // per)
        def _(b):
            @pl.when(b >= 2)
            def _():
                put(c, b - 2).wait()

            @pl.loop(0, per)
            def _(g):
                i0 = pl.multiple_of((b * per + g) * G8, G8)
                v = O[:, pl.ds(i0, G8), :]
                v = v - jnp.mean(v, axis=0, keepdims=True)
                var = jnp.mean(v * v, axis=0, keepdims=True)
                v = v * lax.rsqrt(var + 1e-5) * so[...]
                st[b % 2, g] = v.reshape(ch * G8, v.shape[2]).astype(BF16)

            put(c, b).start()

        put(c, n_g // per - 2).wait()
        put(c, n_g // per - 1).wait()

    @pl.loop(0, 2)
    def _(c):
        @pl.loop(0, nch)
        def _(j):
            p_in(c, j).wait_send()

            @pl.when(mid)
            def _():
                p_out(c, j).wait_send()
                for n in range(3):
                    fwd(n, c, j).wait_send()

            @pl.when(owner)
            def _():
                for t in range(4):
                    rx_c(c, t, j).wait_send()
                    rx_p(c, t, j).wait_send()

            @pl.when(relay)
            def _():
                for t in range(4):
                    rx_f(c, t, j).wait_send()


def spread(mat):
    eye = jnp.eye(G8, dtype=mat.dtype)
    n_o, n_c = mat.shape
    return (mat[:, None, None, :] * eye[None, :, :, None]).reshape(n_o * G8, G8 * n_c)


def solution(mesh):
    nch = 4

    def device_fn(z_one, z_two, mask_one, mask_two, ln_in_scale, w_a, w_a_gate, w_b, w_b_gate, w_gate, w_out, ln_out_scale):
        n_i, n_k, ch = z_one.shape
        zt = [jnp.swapaxes(v, 1, 2) for v in (z_one, z_two)]
        s_in = jnp.broadcast_to(ln_in_scale.astype(F32)[None, :, None], (1, ch, n_k))
        s_out = jnp.broadcast_to(ln_out_scale.astype(F32)[:, None, None], (ch, G8, n_k))

        def pair(w, wg):
            both = jnp.stack([w.T, wg.T]) * jnp.asarray(0.5, BF16)
            both = both.reshape(2, 2, ch // 2, ch).transpose(1, 0, 2, 3).reshape(2 * ch, ch)
            return spread(both).reshape(2, ch * G8, ch * G8)

        wa, wb = pair(w_a, w_a_gate), pair(w_b, w_b_gate)
        eye = jnp.eye(G8, dtype=BF16)
        wgt = w_gate.T * jnp.asarray(0.5, BF16)
        wot = w_out.T * jnp.asarray(0.5, BF16)
        wgk = (eye[:, None, :, None] * wgt[None, :, None, :]).reshape(G8 * ch, G8 * ch)
        wok = (eye[:, None, None, :] * wot[None, :, :, None]).reshape(G8 * ch, ch * G8)

        br = 16
        zspec = pl.BlockSpec((br, ch, n_k), lambda i: (i, 0, 0))
        mspec = pl.BlockSpec((br, n_k), lambda i: (i, 0))
        sspec = pl.BlockSpec((1, ch, n_k), lambda i: (0, 0, 0))
        xm = pl.pallas_call(
            norm_kernel,
            grid=(n_i // br,),
            in_specs=[zspec, zspec, mspec, mspec, sspec],
            out_specs=pl.BlockSpec((2, 1, br, ch, n_k), lambda i: (0, 0, i, 0, 0)),
            out_shape=jax.ShapeDtypeStruct((2, 4, n_i, ch, n_k), BF16),
            name="norm_in",
        )(zt[0], zt[1], mask_one, mask_two, s_in)

        n_g = n_i // G8
        anyspec = pl.BlockSpec(memory_space=pl.ANY)
        vspec = pl.BlockSpec(memory_space=pltpu.VMEM)
        dma = pltpu.SemaphoreType.DMA
        cr = n_i // nch
        on, _, _ = pl.pallas_call(
            functools.partial(tri_kernel, nch, ch),
            out_shape=(
                jax.ShapeDtypeStruct((2, n_g, ch * G8, n_k), BF16),
                jax.ShapeDtypeStruct((2, 4, n_i, ch, n_k), BF16),
                jax.ShapeDtypeStruct((2, 4, n_i, ch, n_k), BF16),
            ),
            in_specs=[anyspec, vspec, vspec, vspec],
            out_specs=(anyspec, anyspec, anyspec),
            input_output_aliases={0: 1},
            scratch_shapes=[
                pltpu.VMEM((ch, n_i, n_k), BF16),
                pltpu.VMEM((ch, n_k, n_k), BF16),
                pltpu.VMEM((ch, n_i, n_k), F32),
                pltpu.VMEM((cr, ch, n_k), BF16),
                pltpu.VMEM((cr, ch, n_k), BF16),
                pltpu.VMEM((2, 4, ch * G8, n_k), BF16),
                dma((2, 3, nch)),
                dma((2, 4, nch)),
                dma((2, nch)),
                dma((2, nch)),
                dma((2, 3, nch)),
                dma((2, 4, nch)),
                dma((2, 4, nch)),
                dma((2,)),
                dma((2,)),
            ],
            compiler_params=pltpu.CompilerParams(has_side_effects=True, vmem_limit_bytes=60 * 1024 * 1024),
            name="triangle",
        )(xm, wa, wb, s_out)

        outs = []
        for crop in range(2):
            out = pl.pallas_call(
                finish_kernel,
                grid=(n_i // br,),
                in_specs=[
                    zspec,
                    pl.BlockSpec((1, br // G8, ch * G8, n_k), lambda i, crop=crop: (crop, i, 0, 0)),
                    sspec,
                    pl.BlockSpec((G8 * ch, G8 * ch), lambda i: (0, 0)),
                    pl.BlockSpec((G8 * ch, ch * G8), lambda i: (0, 0)),
                ],
                out_specs=zspec,
                out_shape=jax.ShapeDtypeStruct((n_i, ch, n_k), BF16),
                name="finish",
            )(zt[crop], on, s_in, wgk, wok)
            outs.append(jnp.swapaxes(out, 1, 2))
        return tuple(outs)

    pair_spec = P(("batch", "row"), "col", None)
    mask_spec = P(("batch", "row"), "col")
    rep = P()
    return jax.shard_map(
        device_fn,
        mesh=mesh,
        in_specs=(pair_spec, pair_spec, mask_spec, mask_spec) + (rep,) * 8,
        out_specs=(pair_spec, pair_spec),
        check_vma=False,
    )
```

```python
import functools

import jax
import jax.numpy as jnp
from jax import lax
from jax.experimental import pallas as pl
from jax.experimental.pallas import tpu as pltpu
from jax.sharding import PartitionSpec as P

MESH = pl.DeviceIdType.MESH
F32 = jnp.float32
BF16 = jnp.bfloat16
G8 = 8


def norm_kernel(z0, z1, m0, m1, s, out):
    scale = s[...]
    for crop, (z, m) in enumerate(((z0, m0), (z1, m1))):
        v = z[...].astype(F32)
        v = v - jnp.mean(v, axis=1, keepdims=True)
        var = jnp.mean(v * v, axis=1, keepdims=True)
        x = (v * lax.rsqrt(var + 1e-5) * scale).astype(BF16)
        mask = m[...].astype(F32)[:, None, :]
        out[crop, 0] = (x.astype(F32) * mask).astype(BF16)


def finish_kernel(z, on, s, wg, wo, out):
    scale = s[...]
    for g in range(z.shape[0] // G8):
        rows = slice(g * G8, (g + 1) * G8)
        zf = z[rows].astype(F32)
        v = zf - jnp.mean(zf, axis=1, keepdims=True)
        var = jnp.mean(v * v, axis=1, keepdims=True)
        x = (v * lax.rsqrt(var + 1e-5) * scale).astype(BF16)
        k = x.shape[1] * G8
        gate = jnp.dot(wg[...], x.reshape(k, x.shape[2]), preferred_element_type=F32)
        half = jnp.dot(wo[...], on[0, g], preferred_element_type=F32)
        upd = ((1.0 + jnp.tanh(gate)) * half).reshape(zf.shape)
        out[rows] = (zf + upd).astype(BF16)


def tri_kernel(nch, ch, gx_in, wa, wb, so, on, gx, rx, r2, ex, A, B, O, xa, xb, st,
               g_sem, r_sem, r2_sem, t_sem, s_in, s_out, s_f, s_r1, s_r2, s_x, s_t, l_sem, o_sem):
    del gx_in
    z = lax.axis_index("col")
    r = lax.axis_index("row")
    h = z // 2
    zz = z + h * (3 - 2 * z)
    q = r + h * (3 - 2 * r)
    inner = z + 1 - 2 * h
    outer = 3 * h
    partner = r + 1 - 2 * (r % 2)
    cross = 2 - h
    mid = zz == 1
    end = zz == 0
    even = q % 2 == 0
    owner = q == zz
    wide_owner = mid & (q == 1)
    relay = mid & (q == 2)
    rx_here = (mid & (q != 1)) | (end & (q == 2))
    extra = mid & (q < 2)
    has_own = mid | even
    r2_from = mid & ((q == 0) | (q == 3))
    r2_row = (1 - (q // 3)) * partner + (q // 3) * 3 * h
    t_row = (1 - q) * (3 - 3 * h) + q * r
    n_i, n_k = gx.shape[2], gx.shape[4]
    cr = n_i // nch
    n_g = n_i // G8
    per = st.shape[1]
    n_b = n_g // per

    def rows(j):
        return pl.ds(pl.multiple_of(j * cr, cr), cr)

    def gs(c, t, j):
        return gx.at[c, t, rows(j)]

    def rs(c, t, j):
        return rx.at[c, t, rows(j)]

    def r2s(c, t, j):
        return r2.at[c, t, rows(j)]

    def cp(src, dst, ssem, rsem, col, row):
        return pltpu.make_async_remote_copy(src_ref=src, dst_ref=dst, send_sem=ssem, recv_sem=rsem,
                                            device_id={"col": col, "row": row}, device_id_type=MESH)

    def p_in(c, j):
        return cp(gs(c, 0, j), gs(c, 1 + zz, j), s_in.at[c, j], g_sem.at[c, zz, j], inner, r)

    def p_out(c, j):
        return cp(gs(c, 0, j), gs(c, 1, j), s_out.at[c, j], g_sem.at[c, 0, j], outer, r)

    def fwd(n, c, j):
        src, dst, col = ((1, 3, inner), (2, 2, outer), (3, 3, outer))[n]
        return cp(gs(c, src, j), gs(c, dst, j), s_f.at[c, n, j], g_sem.at[c, dst - 1, j], col, r)

    def wait_g(c, t, j):
        cp(gs(c, t, j), gs(c, t, j), s_in.at[c, j], g_sem.at[c, t - 1, j], z, r).wait_recv()

    def rx_p(c, t, j):
        return cp(gs(c, t, j), rs(c, t, j), s_r1.at[c, t, j], r_sem.at[c, t, j], z, partner)

    def rx_c(c, t, j):
        return cp(gs(c, t, j), rs(c, t, j), s_r2.at[c, t, j], r_sem.at[c, t, j], z, cross)

    def rx_f(c, t, j):
        return cp(rs(c, t, j), rs(c, t, j), s_r1.at[c, t, j], r_sem.at[c, t, j], z, partner)

    def r2_c(c, t, j):
        return cp(gs(c, t, j), r2s(c, t, j), s_x.at[c, t, j], r2_sem.at[c, t, j], z, r2_row)

    def tile(ref, c, b):
        return ref.at[c, pl.ds(pl.multiple_of(b * per, per), per)]

    def t_c(c, b):
        return cp(tile(ex, c, b), tile(on, c, b), s_t.at[c, b], t_sem.at[c, b], outer, t_row)

    def side_sends(c, t, j):
        @pl.when(owner)
        def _():
            rx_c(c, t, j).start()

        @pl.when(wide_owner)
        def _():
            rx_p(c, t, j).start()

        @pl.when(r2_from)
        def _():
            r2_c(c, t, j).start()

    @pl.loop(0, nch)
    def _(j):
        p_in(0, j).start()

        @pl.when(mid & even)
        def _():
            p_out(0, j).start()

        @pl.when(end)
        def _():
            p_in(1, j).start()

    def comm(c, t, j):
        @pl.when((c == 0) & (t == 0))
        def _():
            side_sends(0, 0, j)

        @pl.when((c == 0) & (t == 2))
        def _():
            side_sends(1, 0, j)

            @pl.when(mid)
            def _():
                p_in(1, j).start()

        @pl.when((t == 1) & mid)
        def _():
            wait_g(c, 1, j)
            fwd(0, c, j).start()
            side_sends(c, 1, j)
            wait_g(c, 2, j)

            @pl.when(even)
            def _():
                fwd(1, c, j).start()

            side_sends(c, 2, j)

        @pl.when((t == 3) & mid)
        def _():
            wait_g(c, 3, j)
            side_sends(c, 3, j)

            @pl.when(even)
            def _():
                fwd(2, c, j).start()

                @pl.when(c == 0)
                def _():
                    p_out(1, j).start()

        @pl.when((t > 0) & end)
        def _():
            for tt in (1, 2, 3):
                @pl.when(t == tt)
                def _():
                    wait_g(c, tt, j)
                    side_sends(c, tt, j)

    half = wa.shape[1] // 2

    def project(src, w, dst, j):
        @pl.loop(0, cr // 16)
        def _(s):
            xs = src[pl.ds(pl.multiple_of(s * 16, 16), 16)]
            x0 = xs[:G8].reshape(G8 * ch, n_k)
            x1 = xs[G8:].reshape(G8 * ch, n_k)
            i0 = pl.multiple_of(j * cr + s * 16, 16)
            nc = half // G8
            for p in range(w.shape[0]):
                parts = []
                for xg in (x0, x1):
                    res = jnp.dot(w[p], xg, preferred_element_type=F32)
                    val = res[:half] * (1.0 + jnp.tanh(res[half:]))
                    parts.append(val.reshape(nc, G8, n_k))
                dst[p * nc:(p + 1) * nc, pl.ds(i0, 16), :] = jnp.concatenate(parts, axis=1).astype(BF16)

    def load(ref, c, t, j, dst, n):
        return pltpu.make_async_copy(ref.at[c, t, rows(j)], dst, l_sem.at[n])

    def steps(c, t, p):
        a_r2 = (p == 0) & (q == 0)
        b_r2 = (p == 0) & (q == 1)
        b_rx = (p == 1) & rx_here
        a_new = (p == 0) | jnp.logical_not(extra & (q == 1))

        @pl.loop(0, nch)
        def _(j):
            @pl.when((p == 0) | jnp.logical_not(extra))
            def _():
                comm(c, t, j)

            @pl.when(jnp.logical_not(b_rx | b_r2))
            def _():
                load(gx, c, t, j, xb, 1).start()

            @pl.when(a_new)
            def _():
                @pl.when(a_r2)
                def _():
                    r2_c(c, t, j).wait_recv()
                    load(r2, c, t, j, xa, 0).start()

                @pl.when(jnp.logical_not(a_r2))
                def _():
                    load(gx, c, t, j, xa, 0).start()

                load(gx, c, t, j, xa, 0).wait()
                project(xa, wa, A, j)

            @pl.when(b_r2)
            def _():
                r2_c(c, t, j).wait_recv()
                load(r2, c, t, j, xb, 1).start()

            @pl.when(b_rx)
            def _():
                rx_p(c, t, j).wait_recv()

                @pl.when(relay)
                def _():
                    rx_f(c, t, j).start()

                load(rx, c, t, j, xb, 1).start()

            load(gx, c, t, j, xb, 1).wait()
            project(xb, wb, B, j)

        @pl.loop(0, ch)
        def _(k):
            prod = lax.dot_general(A[k], B[k], (((1,), (1,)), ((), ())), preferred_element_type=F32)

            @pl.when(t == 0)
            def _():
                O[p, k] = prod

            @pl.when(t > 0)
            def _():
                O[p, k] += prod

    def put(c, b, p):
        src = st.at[b % 2]

        @pl.when(p == 0)
        def _():
            pltpu.make_async_copy(src, tile(ex, c, b), o_sem.at[b % 2]).start()

        @pl.when(p == 1)
        def _():
            pltpu.make_async_copy(src, tile(on, c, b), o_sem.at[b % 2]).start()

    def put_done(c, b, p):
        pltpu.make_async_copy(st.at[b % 2], tile(ex, c, b), o_sem.at[b % 2]).wait()

        @pl.when(p == 0)
        def _():
            t_c(c, b).start()

    def close(c, p):
        @pl.loop(0, n_b)
        def _(b):
            @pl.loop(0, per)
            def _(g):
                i0 = pl.multiple_of((b * per + g) * G8, G8)
                v = O[p, :, pl.ds(i0, G8), :]
                v = v - jnp.mean(v, axis=0, keepdims=True)
                var = jnp.mean(v * v, axis=0, keepdims=True)
                v = v * lax.rsqrt(var + 1e-5) * so[...]
                st[b % 2, g] = v.reshape(ch * G8, v.shape[2]).astype(BF16)

            put(c, b, p)

            @pl.when(b >= 1)
            def _():
                put_done(c, b - 1, p)

        put_done(c, n_b - 1, p)

    @pl.when(has_own)
    def _():
        @pl.loop(0, 2)
        def _(c):
            @pl.loop(0, 4)
            def _(t):
                @pl.loop(0, 2)
                def _(p):
                    @pl.when((p == 1) | extra)
                    def _():
                        steps(c, t, p)

                        @pl.when(t == 3)
                        def _():
                            close(c, p)

    @pl.loop(0, 2)
    def _(c):
        @pl.when(end & jnp.logical_not(even))
        def _():
            @pl.loop(0, n_b)
            def _(b):
                t_c(c, b).wait_recv()

        @pl.when(extra)
        def _():
            @pl.loop(0, n_b)
            def _(b):
                t_c(c, b).wait_send()

        @pl.loop(0, nch)
        def _(j):
            p_in(c, j).wait_send()

            @pl.when(mid)
            def _():
                fwd(0, c, j).wait_send()

                @pl.when(even)
                def _():
                    p_out(c, j).wait_send()
                    fwd(1, c, j).wait_send()
                    fwd(2, c, j).wait_send()

            @pl.loop(0, 4)
            def _(t):
                @pl.when(owner)
                def _():
                    rx_c(c, t, j).wait_send()

                @pl.when(wide_owner)
                def _():
                    rx_p(c, t, j).wait_send()

                @pl.when(relay)
                def _():
                    rx_f(c, t, j).wait_send()

                @pl.when(r2_from)
                def _():
                    r2_c(c, t, j).wait_send()


def spread(mat):
    eye = jnp.eye(G8, dtype=mat.dtype)
    n_o, n_c = mat.shape
    return (mat[:, None, None, :] * eye[None, :, :, None]).reshape(n_o * G8, G8 * n_c)


def solution(mesh):
    nch = 4

    def device_fn(z_one, z_two, mask_one, mask_two, ln_in_scale, w_a, w_a_gate, w_b, w_b_gate, w_gate, w_out, ln_out_scale):
        n_i, n_k, ch = z_one.shape
        zt = [jnp.swapaxes(v, 1, 2) for v in (z_one, z_two)]
        s_in = jnp.broadcast_to(ln_in_scale.astype(F32)[None, :, None], (1, ch, n_k))
        s_out = jnp.broadcast_to(ln_out_scale.astype(F32)[:, None, None], (ch, G8, n_k))

        def pair(w, wg):
            both = jnp.stack([w.T, wg.T]) * jnp.asarray(0.5, BF16)
            both = both.reshape(2, 2, ch // 2, ch).transpose(1, 0, 2, 3).reshape(2 * ch, ch)
            return spread(both).reshape(2, ch * G8, ch * G8)

        wa, wb = pair(w_a, w_a_gate), pair(w_b, w_b_gate)
        eye = jnp.eye(G8, dtype=BF16)
        wgt = w_gate.T * jnp.asarray(0.5, BF16)
        wot = w_out.T * jnp.asarray(0.5, BF16)
        wgk = (eye[:, None, :, None] * wgt[None, :, None, :]).reshape(G8 * ch, G8 * ch)
        wok = (eye[:, None, None, :] * wot[None, :, :, None]).reshape(G8 * ch, ch * G8)

        br = 16
        zspec = pl.BlockSpec((br, ch, n_k), lambda i: (i, 0, 0))
        mspec = pl.BlockSpec((br, n_k), lambda i: (i, 0))
        sspec = pl.BlockSpec((1, ch, n_k), lambda i: (0, 0, 0))
        xm = pl.pallas_call(
            norm_kernel,
            grid=(n_i // br,),
            in_specs=[zspec, zspec, mspec, mspec, sspec],
            out_specs=pl.BlockSpec((2, 1, br, ch, n_k), lambda i: (0, 0, i, 0, 0)),
            out_shape=jax.ShapeDtypeStruct((2, 4, n_i, ch, n_k), BF16),
            name="norm_in",
        )(zt[0], zt[1], mask_one, mask_two, s_in)

        n_g = n_i // G8
        anyspec = pl.BlockSpec(memory_space=pl.ANY)
        vspec = pl.BlockSpec(memory_space=pltpu.VMEM)
        dma = pltpu.SemaphoreType.DMA
        cr = n_i // nch
        per = 4
        on, _, _, _, _ = pl.pallas_call(
            functools.partial(tri_kernel, nch, ch),
            out_shape=(
                jax.ShapeDtypeStruct((2, n_g, ch * G8, n_k), BF16),
                jax.ShapeDtypeStruct((2, 4, n_i, ch, n_k), BF16),
                jax.ShapeDtypeStruct((2, 4, n_i, ch, n_k), BF16),
                jax.ShapeDtypeStruct((2, 4, n_i, ch, n_k), BF16),
                jax.ShapeDtypeStruct((2, n_g, ch * G8, n_k), BF16),
            ),
            in_specs=[anyspec, vspec, vspec, vspec],
            out_specs=(anyspec,) * 5,
            input_output_aliases={0: 1},
            scratch_shapes=[
                pltpu.VMEM((ch, n_i, n_k), BF16),
                pltpu.VMEM((ch, n_k, n_k), BF16),
                pltpu.VMEM((2, ch, n_i, n_k), F32),
                pltpu.VMEM((cr, ch, n_k), BF16),
                pltpu.VMEM((cr, ch, n_k), BF16),
                pltpu.VMEM((2, per, ch * G8, n_k), BF16),
                dma((2, 3, nch)),
                dma((2, 4, nch)),
                dma((2, 4, nch)),
                dma((2, n_g // per)),
                dma((2, nch)),
                dma((2, nch)),
                dma((2, 3, nch)),
                dma((2, 4, nch)),
                dma((2, 4, nch)),
                dma((2, 4, nch)),
                dma((2, n_g // per)),
                dma((2,)),
                dma((2,)),
            ],
            compiler_params=pltpu.CompilerParams(has_side_effects=True, vmem_limit_bytes=60 * 1024 * 1024),
            name="triangle",
        )(xm, wa, wb, s_out)

        outs = []
        for crop in range(2):
            out = pl.pallas_call(
                finish_kernel,
                grid=(n_i // br,),
                in_specs=[
                    zspec,
                    pl.BlockSpec((1, br // G8, ch * G8, n_k), lambda i, crop=crop: (crop, i, 0, 0)),
                    sspec,
                    pl.BlockSpec((G8 * ch, G8 * ch), lambda i: (0, 0)),
                    pl.BlockSpec((G8 * ch, ch * G8), lambda i: (0, 0)),
                ],
                out_specs=zspec,
                out_shape=jax.ShapeDtypeStruct((n_i, ch, n_k), BF16),
                name="finish",
            )(zt[crop], on, s_in, wgk, wok)
            outs.append(jnp.swapaxes(out, 1, 2))
        return tuple(outs)

    pair_spec = P(("batch", "row"), "col", None)
    mask_spec = P(("batch", "row"), "col")
    rep = P()
    return jax.shard_map(
        device_fn,
        mesh=mesh,
        in_specs=(pair_spec, pair_spec, mask_spec, mask_spec) + (rep,) * 8,
        out_specs=(pair_spec, pair_spec),
        check_vma=False,
    )
```

```python
import functools

import jax
import jax.numpy as jnp
from jax import lax
from jax.experimental import pallas as pl
from jax.experimental.pallas import tpu as pltpu
from jax.sharding import PartitionSpec as P

MESH = pl.DeviceIdType.MESH
F32 = jnp.float32
BF16 = jnp.bfloat16
G8 = 8


def norm_kernel(z0, z1, m0, m1, s, out):
    scale = s[...]
    for crop, (z, m) in enumerate(((z0, m0), (z1, m1))):
        v = z[...].astype(F32)
        v = v - jnp.mean(v, axis=1, keepdims=True)
        var = jnp.mean(v * v, axis=1, keepdims=True)
        x = (v * lax.rsqrt(var + 1e-5) * scale).astype(BF16)
        mask = m[...].astype(F32)[:, None, :]
        out[crop, 0] = (x.astype(F32) * mask).astype(BF16)


def finish_kernel(z, on, s, wg, wo, out):
    scale = s[...]
    for g in range(z.shape[0] // G8):
        rows = slice(g * G8, (g + 1) * G8)
        zf = z[rows].astype(F32)
        v = zf - jnp.mean(zf, axis=1, keepdims=True)
        var = jnp.mean(v * v, axis=1, keepdims=True)
        x = (v * lax.rsqrt(var + 1e-5) * scale).astype(BF16)
        k = x.shape[1] * G8
        gate = jnp.dot(wg[...], x.reshape(k, x.shape[2]), preferred_element_type=F32)
        half = jnp.dot(wo[...], on[0, g], preferred_element_type=F32)
        upd = ((1.0 + jnp.tanh(gate)) * half).reshape(zf.shape)
        out[rows] = (zf + upd).astype(BF16)


def tri_kernel(nch, ch, gx_in, wa, wb, so, on, gx, rx, r2, ex, A, B, O, xa, xb, st,
               g_sem, r_sem, r2_sem, t_sem, s_in, s_out, s_f, s_r1, s_r2, s_x, s_t, l_sem, o_sem):
    del gx_in
    z = lax.axis_index("col")
    r = lax.axis_index("row")
    h = z // 2
    zz = z + h * (3 - 2 * z)
    q = r + h * (3 - 2 * r)
    inner = z + 1 - 2 * h
    outer = 3 * h
    partner = r + 1 - 2 * (r % 2)
    cross = 2 - h
    mid = zz == 1
    end = zz == 0
    even = q % 2 == 0
    owner = q == zz
    wide_owner = mid & (q == 1)
    relay = mid & (q == 2)
    rx_here = (mid & (q != 1)) | (end & (q == 2))
    extra = mid & (q < 2)
    has_own = mid | even
    r2_from = mid & ((q == 0) | (q == 3))
    r2_row = (1 - (q // 3)) * partner + (q // 3) * 3 * h
    t_row = (1 - q) * (3 - 3 * h) + q * r
    n_i, n_k = gx.shape[2], gx.shape[4]
    cr = n_i // nch
    n_g = n_i // G8
    per = st.shape[1]
    n_b = n_g // per

    def rows(j):
        return pl.ds(pl.multiple_of(j * cr, cr), cr)

    def gs(c, t, j):
        return gx.at[c, t, rows(j)]

    def rs(c, t, j):
        return rx.at[c, t, rows(j)]

    def r2s(c, t, j):
        return r2.at[c, t, rows(j)]

    def cp(src, dst, ssem, rsem, col, row):
        return pltpu.make_async_remote_copy(src_ref=src, dst_ref=dst, send_sem=ssem, recv_sem=rsem,
                                            device_id={"col": col, "row": row}, device_id_type=MESH)

    def p_in(c, j):
        return cp(gs(c, 0, j), gs(c, 1 + zz, j), s_in.at[c, j], g_sem.at[c, zz, j], inner, r)

    def p_out(c, j):
        return cp(gs(c, 0, j), gs(c, 1, j), s_out.at[c, j], g_sem.at[c, 0, j], outer, r)

    def fwd(n, c, j):
        src, dst, col = ((1, 3, inner), (2, 2, outer), (3, 3, outer))[n]
        return cp(gs(c, src, j), gs(c, dst, j), s_f.at[c, n, j], g_sem.at[c, dst - 1, j], col, r)

    def wait_g(c, t, j):
        cp(gs(c, t, j), gs(c, t, j), s_in.at[c, j], g_sem.at[c, t - 1, j], z, r).wait_recv()

    def rx_p(c, t, j):
        return cp(gs(c, t, j), rs(c, t, j), s_r1.at[c, t, j], r_sem.at[c, t, j], z, partner)

    def rx_c(c, t, j):
        return cp(gs(c, t, j), rs(c, t, j), s_r2.at[c, t, j], r_sem.at[c, t, j], z, cross)

    def rx_f(c, t, j):
        return cp(rs(c, t, j), rs(c, t, j), s_r1.at[c, t, j], r_sem.at[c, t, j], z, partner)

    def r2_c(c, t, j):
        return cp(gs(c, t, j), r2s(c, t, j), s_x.at[c, t, j], r2_sem.at[c, t, j], z, r2_row)

    def tile(ref, c, b):
        return ref.at[c, pl.ds(pl.multiple_of(b * per, per), per)]

    def t_c(c, b):
        return cp(tile(ex, c, b), tile(on, c, b), s_t.at[c, b], t_sem.at[c, b], outer, t_row)

    def side_sends(c, t, j):
        @pl.when(owner)
        def _():
            rx_c(c, t, j).start()

        @pl.when(wide_owner)
        def _():
            rx_p(c, t, j).start()

        @pl.when(r2_from)
        def _():
            r2_c(c, t, j).start()

    @pl.loop(0, nch)
    def _(j):
        p_in(0, j).start()
        side_sends(0, 0, j)

        @pl.when(mid & even)
        def _():
            p_out(0, j).start()

        @pl.when(end)
        def _():
            p_in(1, j).start()

    def comm_near(c, j):
        wait_g(c, 1, j)

        @pl.when(mid)
        def _():
            fwd(0, c, j).start()

        side_sends(c, 1, j)
        wait_g(c, 2, j)

        @pl.when(mid & even)
        def _():
            fwd(1, c, j).start()

        side_sends(c, 2, j)

    def comm_far(c, j):
        @pl.when((c == 0) & mid)
        def _():
            p_in(1, j).start()

        wait_g(c, 3, j)

        @pl.when(mid & even)
        def _():
            fwd(2, c, j).start()

        side_sends(c, 3, j)

        @pl.when(c == 0)
        def _():
            side_sends(1, 0, j)

            @pl.when(mid & even)
            def _():
                p_out(1, j).start()

    def comm(c, t, j):
        u = t * nch + j
        v = u % 8
        jj = v - 3 + (6 - v) // 4
        hit = (v == 2) | ((v >= 4) & (v <= 6))

        @pl.when(hit & (u < 8))
        def _():
            comm_near(c, jj)

        @pl.when(hit & (u >= 8))
        def _():
            comm_far(c, jj)

    half = wa.shape[1] // 2

    def project(src, w, dst, j):
        @pl.loop(0, cr // 16)
        def _(s):
            xs = src[pl.ds(pl.multiple_of(s * 16, 16), 16)]
            x0 = xs[:G8].reshape(G8 * ch, n_k)
            x1 = xs[G8:].reshape(G8 * ch, n_k)
            i0 = pl.multiple_of(j * cr + s * 16, 16)
            nc = half // G8
            for p in range(w.shape[0]):
                parts = []
                for xg in (x0, x1):
                    res = jnp.dot(w[p], xg, preferred_element_type=F32)
                    val = res[:half] * (1.0 + jnp.tanh(res[half:]))
                    parts.append(val.reshape(nc, G8, n_k))
                dst[p * nc:(p + 1) * nc, pl.ds(i0, 16), :] = jnp.concatenate(parts, axis=1).astype(BF16)

    def load(ref, c, t, j, dst, n):
        return pltpu.make_async_copy(ref.at[c, t, rows(j)], dst, l_sem.at[n])

    def steps(c, t, p):
        a_r2 = (p == 0) & (q == 0)
        b_r2 = (p == 0) & (q == 1)
        b_rx = (p == 1) & rx_here
        a_new = (p == 0) | jnp.logical_not(extra & (q == 1))

        @pl.loop(0, nch)
        def _(j):
            @pl.when((p == 0) | jnp.logical_not(extra))
            def _():
                comm(c, t, j)

            @pl.when(jnp.logical_not(b_rx | b_r2))
            def _():
                load(gx, c, t, j, xb, 1).start()

            @pl.when(a_new)
            def _():
                @pl.when(a_r2)
                def _():
                    r2_c(c, t, j).wait_recv()
                    load(r2, c, t, j, xa, 0).start()

                @pl.when(jnp.logical_not(a_r2))
                def _():
                    load(gx, c, t, j, xa, 0).start()

                load(gx, c, t, j, xa, 0).wait()
                project(xa, wa, A, j)

            @pl.when(b_r2)
            def _():
                r2_c(c, t, j).wait_recv()
                load(r2, c, t, j, xb, 1).start()

            @pl.when(b_rx)
            def _():
                rx_p(c, t, j).wait_recv()

                @pl.when(relay)
                def _():
                    rx_f(c, t, j).start()

                load(rx, c, t, j, xb, 1).start()

            load(gx, c, t, j, xb, 1).wait()
            project(xb, wb, B, j)

        @pl.loop(0, ch)
        def _(k):
            prod = lax.dot_general(A[k], B[k], (((1,), (1,)), ((), ())), preferred_element_type=F32)

            @pl.when(t == 0)
            def _():
                O[p, k] = prod

            @pl.when(t > 0)
            def _():
                O[p, k] += prod

    def put(c, b, p):
        src = st.at[b % 2]

        @pl.when(p == 0)
        def _():
            pltpu.make_async_copy(src, tile(ex, c, b), o_sem.at[b % 2]).start()

        @pl.when(p == 1)
        def _():
            pltpu.make_async_copy(src, tile(on, c, b), o_sem.at[b % 2]).start()

    def put_done(c, b, p):
        pltpu.make_async_copy(st.at[b % 2], tile(ex, c, b), o_sem.at[b % 2]).wait()

        @pl.when(p == 0)
        def _():
            t_c(c, b).start()

    def close(c, p):
        @pl.loop(0, n_b)
        def _(b):
            @pl.loop(0, per)
            def _(g):
                i0 = pl.multiple_of((b * per + g) * G8, G8)
                v = O[p, :, pl.ds(i0, G8), :]
                v = v - jnp.mean(v, axis=0, keepdims=True)
                var = jnp.mean(v * v, axis=0, keepdims=True)
                v = v * lax.rsqrt(var + 1e-5) * so[...]
                st[b % 2, g] = v.reshape(ch * G8, v.shape[2]).astype(BF16)

            put(c, b, p)

            @pl.when(b >= 1)
            def _():
                put_done(c, b - 1, p)

        put_done(c, n_b - 1, p)

    @pl.when(has_own)
    def _():
        @pl.loop(0, 2)
        def _(c):
            @pl.loop(0, 4)
            def _(t):
                @pl.loop(0, 2)
                def _(p):
                    @pl.when((p == 1) | extra)
                    def _():
                        steps(c, t, p)

                        @pl.when(t == 3)
                        def _():
                            close(c, p)

    @pl.loop(0, 2)
    def _(c):
        @pl.when(end & jnp.logical_not(even))
        def _():
            @pl.loop(0, n_b)
            def _(b):
                t_c(c, b).wait_recv()

        @pl.when(extra)
        def _():
            @pl.loop(0, n_b)
            def _(b):
                t_c(c, b).wait_send()

        @pl.loop(0, nch)
        def _(j):
            p_in(c, j).wait_send()

            @pl.when(mid)
            def _():
                fwd(0, c, j).wait_send()

                @pl.when(even)
                def _():
                    p_out(c, j).wait_send()
                    fwd(1, c, j).wait_send()
                    fwd(2, c, j).wait_send()

            @pl.loop(0, 4)
            def _(t):
                @pl.when(owner)
                def _():
                    rx_c(c, t, j).wait_send()

                @pl.when(wide_owner)
                def _():
                    rx_p(c, t, j).wait_send()

                @pl.when(relay)
                def _():
                    rx_f(c, t, j).wait_send()

                @pl.when(r2_from)
                def _():
                    r2_c(c, t, j).wait_send()


def spread(mat):
    eye = jnp.eye(G8, dtype=mat.dtype)
    n_o, n_c = mat.shape
    return (mat[:, None, None, :] * eye[None, :, :, None]).reshape(n_o * G8, G8 * n_c)


def solution(mesh):
    nch = 4

    def device_fn(z_one, z_two, mask_one, mask_two, ln_in_scale, w_a, w_a_gate, w_b, w_b_gate, w_gate, w_out, ln_out_scale):
        n_i, n_k, ch = z_one.shape
        zt = [jnp.swapaxes(v, 1, 2) for v in (z_one, z_two)]
        s_in = jnp.broadcast_to(ln_in_scale.astype(F32)[None, :, None], (1, ch, n_k))
        s_out = jnp.broadcast_to(ln_out_scale.astype(F32)[:, None, None], (ch, G8, n_k))

        def pair(w, wg):
            both = jnp.stack([w.T, wg.T]) * jnp.asarray(0.5, BF16)
            both = both.reshape(2, 2, ch // 2, ch).transpose(1, 0, 2, 3).reshape(2 * ch, ch)
            return spread(both).reshape(2, ch * G8, ch * G8)

        wa, wb = pair(w_a, w_a_gate), pair(w_b, w_b_gate)
        eye = jnp.eye(G8, dtype=BF16)
        wgt = w_gate.T * jnp.asarray(0.5, BF16)
        wot = w_out.T * jnp.asarray(0.5, BF16)
        wgk = (eye[:, None, :, None] * wgt[None, :, None, :]).reshape(G8 * ch, G8 * ch)
        wok = (eye[:, None, None, :] * wot[None, :, :, None]).reshape(G8 * ch, ch * G8)

        br = 16
        zspec = pl.BlockSpec((br, ch, n_k), lambda i: (i, 0, 0))
        mspec = pl.BlockSpec((br, n_k), lambda i: (i, 0))
        sspec = pl.BlockSpec((1, ch, n_k), lambda i: (0, 0, 0))
        xm = pl.pallas_call(
            norm_kernel,
            grid=(n_i // br,),
            in_specs=[zspec, zspec, mspec, mspec, sspec],
            out_specs=pl.BlockSpec((2, 1, br, ch, n_k), lambda i: (0, 0, i, 0, 0)),
            out_shape=jax.ShapeDtypeStruct((2, 4, n_i, ch, n_k), BF16),
            name="norm_in",
        )(zt[0], zt[1], mask_one, mask_two, s_in)

        n_g = n_i // G8
        anyspec = pl.BlockSpec(memory_space=pl.ANY)
        vspec = pl.BlockSpec(memory_space=pltpu.VMEM)
        dma = pltpu.SemaphoreType.DMA
        cr = n_i // nch
        per = 4
        on, _, _, _, _ = pl.pallas_call(
            functools.partial(tri_kernel, nch, ch),
            out_shape=(
                jax.ShapeDtypeStruct((2, n_g, ch * G8, n_k), BF16),
                jax.ShapeDtypeStruct((2, 4, n_i, ch, n_k), BF16),
                jax.ShapeDtypeStruct((2, 4, n_i, ch, n_k), BF16),
                jax.ShapeDtypeStruct((2, 4, n_i, ch, n_k), BF16),
                jax.ShapeDtypeStruct((2, n_g, ch * G8, n_k), BF16),
            ),
            in_specs=[anyspec, vspec, vspec, vspec],
            out_specs=(anyspec,) * 5,
            input_output_aliases={0: 1},
            scratch_shapes=[
                pltpu.VMEM((ch, n_i, n_k), BF16),
                pltpu.VMEM((ch, n_k, n_k), BF16),
                pltpu.VMEM((2, ch, n_i, n_k), F32),
                pltpu.VMEM((cr, ch, n_k), BF16),
                pltpu.VMEM((cr, ch, n_k), BF16),
                pltpu.VMEM((2, per, ch * G8, n_k), BF16),
                dma((2, 3, nch)),
                dma((2, 4, nch)),
                dma((2, 4, nch)),
                dma((2, n_g // per)),
                dma((2, nch)),
                dma((2, nch)),
                dma((2, 3, nch)),
                dma((2, 4, nch)),
                dma((2, 4, nch)),
                dma((2, 4, nch)),
                dma((2, n_g // per)),
                dma((2,)),
                dma((2,)),
            ],
            compiler_params=pltpu.CompilerParams(has_side_effects=True, vmem_limit_bytes=60 * 1024 * 1024),
            name="triangle",
        )(xm, wa, wb, s_out)

        outs = []
        for crop in range(2):
            out = pl.pallas_call(
                finish_kernel,
                grid=(n_i // br,),
                in_specs=[
                    zspec,
                    pl.BlockSpec((1, br // G8, ch * G8, n_k), lambda i, crop=crop: (crop, i, 0, 0)),
                    sspec,
                    pl.BlockSpec((G8 * ch, G8 * ch), lambda i: (0, 0)),
                    pl.BlockSpec((G8 * ch, ch * G8), lambda i: (0, 0)),
                ],
                out_specs=zspec,
                out_shape=jax.ShapeDtypeStruct((n_i, ch, n_k), BF16),
                name="finish",
            )(zt[crop], on, s_in, wgk, wok)
            outs.append(jnp.swapaxes(out, 1, 2))
        return tuple(outs)

    pair_spec = P(("batch", "row"), "col", None)
    mask_spec = P(("batch", "row"), "col")
    rep = P()
    return jax.shard_map(
        device_fn,
        mesh=mesh,
        in_specs=(pair_spec, pair_spec, mask_spec, mask_spec) + (rep,) * 8,
        out_specs=(pair_spec, pair_spec),
        check_vma=False,
    )
```

```python
import functools

import jax
import jax.numpy as jnp
from jax import lax
from jax.experimental import pallas as pl
from jax.experimental.pallas import tpu as pltpu
from jax.sharding import PartitionSpec as P

MESH = pl.DeviceIdType.MESH
F32 = jnp.float32
BF16 = jnp.bfloat16
G8 = 8


def grow(w, first, count, rows_inner, cols_inner):
    k, m = w.shape
    i_r, i_m = (lax.broadcasted_iota(jnp.int32, (G8 * count, m), d) for d in (0, 1))
    i_k, i_c = (lax.broadcasted_iota(jnp.int32, (k, G8 * k), d) for d in (0, 1))
    pick_r = ((i_r // G8 if rows_inner else i_r % count) + first == i_m).astype(F32).astype(BF16)
    pick_c = ((i_c // G8 if cols_inner else i_c % k) == i_k).astype(F32).astype(BF16)
    big = lax.dot_general(pick_r, w, (((1,), (1,)), ((), ())), preferred_element_type=F32).astype(BF16)
    big = jnp.dot(big, pick_c, preferred_element_type=F32) * 0.5
    b_r, b_c = (lax.broadcasted_iota(jnp.int32, (G8 * count, G8 * k), d) for d in (0, 1))
    row_r = b_r % G8 if rows_inner else b_r // count
    row_c = b_c % G8 if cols_inner else b_c // k
    return jnp.where(row_r == row_c, big, 0.0).astype(BF16)


def layer_norm_row(zf, scale, keep):
    v = zf - jnp.mean(zf, axis=0, keepdims=True)
    rstd = lax.rsqrt(jnp.mean(v * v, axis=0, keepdims=True) + 1e-5)
    if keep is not None:
        rstd = rstd * keep
    return v * rstd * scale


def norm_kernel(z0, z1, m0, m1, s, wa, wag, wb, wbg, wg, wo, out, w_ab, w_g, w_o):
    @pl.when(pl.program_id(0) == 0)
    def _():
        ch = wa.shape[0]
        hc = ch // 2
        for side, ws in enumerate(((wa, wag), (wb, wbg))):
            for p in range(2):
                for kind in range(2):
                    part = slice(kind * hc * G8, (kind + 1) * hc * G8)
                    w_ab[side, p, part, :] = grow(ws[kind][...], p * hc, hc, True, False)
        w_g[...] = grow(wg[...], 0, ch, False, False)
        w_o[...] = grow(wo[...], 0, ch, False, True)

    scale = s[...]
    for crop, (z, m) in enumerate(((z0, m0), (z1, m1))):
        @pl.loop(0, z.shape[0] // G8)
        def _(g):
            i0 = pl.multiple_of(g * G8, G8)
            keep = m[pl.ds(i0, G8), :].astype(F32)
            for d in range(G8):
                x = layer_norm_row(z[i0 + d].astype(F32), scale, keep[d:d + 1])
                out[crop, 0, i0 + d] = x.astype(BF16)


def finish_kernel(z0, z1, on0, on1, s, wg, wo, out0, out1):
    scale = s[...]
    for z, on, out in ((z0, on0, out0), (z1, on1, out1)):
        ch, n_k = z.shape[1:]
        for g in range(z.shape[0] // G8):
            half = jnp.dot(wo[...], on[0, g], preferred_element_type=F32)
            for d in range(0, G8, 4):
                r = g * G8 + d
                x = jnp.concatenate(
                    [layer_norm_row(z[r + e].astype(F32), scale, None).astype(BF16) for e in range(4)], axis=0)
                gate = jnp.dot(wg[:4 * ch, :4 * ch], x, preferred_element_type=F32)
                upd = (1.0 + jnp.tanh(gate)) * half[d * ch:(d + 4) * ch]
                for e in range(4):
                    out[r + e] = (z[r + e].astype(F32) + upd[e * ch:(e + 1) * ch]).astype(BF16)


def tri_kernel(nch, ch, gx_in, w, so, on, gx, rx, r2, ex, AB, O, xb, st,
               g_sem, r_sem, r2_sem, t_sem, s_in, s_out, s_f, s_r1, s_r2, s_x, s_t, l_sem, o_sem):
    del gx_in
    z = lax.axis_index("col")
    r = lax.axis_index("row")
    h = z // 2
    zz = z + h * (3 - 2 * z)
    q = r + h * (3 - 2 * r)
    inner = z + 1 - 2 * h
    outer = 3 * h
    partner = r + 1 - 2 * (r % 2)
    cross = 2 - h
    mid = zz == 1
    end = zz == 0
    even = q % 2 == 0
    owner = q == zz
    wide_owner = mid & (q == 1)
    relay = mid & (q == 2)
    rx_here = (mid & (q != 1)) | (end & (q == 2))
    extra = mid & (q < 2)
    has_own = mid | even
    r2_from = mid & ((q == 0) | (q == 3))
    r2_row = (1 - (q // 3)) * partner + (q // 3) * 3 * h
    t_row = (1 - q) * (3 - 3 * h) + q * r
    n_i, n_k = gx.shape[2], gx.shape[4]
    cr = n_i // nch
    n_g = n_i // G8
    per = st.shape[1]
    n_b = n_g // per

    def rows(j):
        return pl.ds(pl.multiple_of(j * cr, cr), cr)

    def gs(c, t, j):
        return gx.at[c, t, rows(j)]

    def rs(c, t, j):
        return rx.at[c, t, rows(j)]

    def r2s(c, t, j):
        return r2.at[c, t, rows(j)]

    def cp(src, dst, ssem, rsem, col, row):
        return pltpu.make_async_remote_copy(src_ref=src, dst_ref=dst, send_sem=ssem, recv_sem=rsem,
                                            device_id={"col": col, "row": row}, device_id_type=MESH)

    def p_in(c, j):
        return cp(gs(c, 0, j), gs(c, 1 + zz, j), s_in.at[c, j], g_sem.at[c, zz, j], inner, r)

    def p_out(c, j):
        return cp(gs(c, 0, j), gs(c, 1, j), s_out.at[c, j], g_sem.at[c, 0, j], outer, r)

    def fwd(n, c, j):
        src, dst, col = ((1, 3, inner), (2, 2, outer), (3, 3, outer))[n]
        return cp(gs(c, src, j), gs(c, dst, j), s_f.at[c, n, j], g_sem.at[c, dst - 1, j], col, r)

    def wait_g(c, t, j):
        cp(gs(c, t, j), gs(c, t, j), s_in.at[c, j], g_sem.at[c, t - 1, j], z, r).wait_recv()

    def rx_p(c, t, j):
        return cp(gs(c, t, j), rs(c, t, j), s_r1.at[c, t, j], r_sem.at[c, t, j], z, partner)

    def rx_c(c, t, j):
        return cp(gs(c, t, j), rs(c, t, j), s_r2.at[c, t, j], r_sem.at[c, t, j], z, cross)

    def rx_f(c, t, j):
        return cp(rs(c, t, j), rs(c, t, j), s_r1.at[c, t, j], r_sem.at[c, t, j], z, partner)

    def r2_c(c, t, j):
        return cp(gs(c, t, j), r2s(c, t, j), s_x.at[c, t, j], r2_sem.at[c, t, j], z, r2_row)

    def tile(ref, c, b):
        return ref.at[c, pl.ds(pl.multiple_of(b * per, per), per)]

    def t_c(c, b):
        return cp(tile(ex, c, b), tile(on, c, b), s_t.at[c, b], t_sem.at[c, b], outer, t_row)

    def side_sends(c, t, j):
        @pl.when(owner)
        def _():
            rx_c(c, t, j).start()

        @pl.when(wide_owner)
        def _():
            rx_p(c, t, j).start()

        @pl.when(r2_from)
        def _():
            r2_c(c, t, j).start()

    @pl.loop(0, nch)
    def _(j):
        p_in(0, j).start()
        side_sends(0, 0, j)

        @pl.when(mid & even)
        def _():
            p_out(0, j).start()

        @pl.when(end)
        def _():
            p_in(1, j).start()

    def comm_near(c, j):
        wait_g(c, 1, j)

        @pl.when(mid)
        def _():
            fwd(0, c, j).start()

        side_sends(c, 1, j)
        wait_g(c, 2, j)

        @pl.when(mid & even)
        def _():
            fwd(1, c, j).start()

        side_sends(c, 2, j)

    def comm_far(c, j):
        @pl.when((c == 0) & mid)
        def _():
            p_in(1, j).start()

        wait_g(c, 3, j)

        @pl.when(mid & even)
        def _():
            fwd(2, c, j).start()

        side_sends(c, 3, j)

        @pl.when(c == 0)
        def _():
            side_sends(1, 0, j)

            @pl.when(mid & even)
            def _():
                p_out(1, j).start()

    def comm(c, t, j):
        u = t * nch + j
        v = u % 8
        jj = v - 3 + (6 - v) // 4
        hit = (v == 2) | ((v >= 4) & (v <= 6))

        @pl.when(hit & (u < 8))
        def _():
            comm_near(c, jj)

        @pl.when(hit & (u >= 8))
        def _():
            comm_far(c, jj)

    half = w.shape[2] // 2

    def project(buf, sel, j):
        @pl.loop(0, cr // 16)
        def _(s):
            xs = xb[buf, pl.ds(pl.multiple_of(s * 16, 16), 16)]
            x0 = xs[:G8].reshape(G8 * ch, n_k)
            x1 = xs[G8:].reshape(G8 * ch, n_k)
            i0 = pl.multiple_of(j * cr + s * 16, 16)
            nc = half // G8
            for p in range(w.shape[1]):
                parts = []
                for xg in (x0, x1):
                    res = jnp.dot(w[sel, p], xg, preferred_element_type=F32)
                    val = res[:half] * (1.0 + jnp.tanh(res[half:]))
                    parts.append(val.reshape(nc, G8, n_k))
                AB[sel, p * nc:(p + 1) * nc, pl.ds(i0, 16), :] = jnp.concatenate(parts, axis=1).astype(BF16)

    def load(ref, c, t, j, buf):
        return pltpu.make_async_copy(ref.at[c, t, rows(j)], xb.at[buf], l_sem.at[buf])

    def steps(c, t, p):
        first_b = (p == 0) & (q == 0)
        from_r2 = p == 0
        from_rx = (p == 1) & rx_here
        remote = from_r2 | from_rx
        keep_a = (p == 1) & extra & (q == 1)
        sel1 = first_b.astype(jnp.int32)
        sel2 = 1 - sel1
        again = ((p == 0) & extra).astype(jnp.int32)

        @pl.loop(0, nch)
        def _(j):
            @pl.when((p == 0) | jnp.logical_not(extra))
            def _():
                comm(c, t, j)

            @pl.when(from_r2)
            def _():
                r2_c(c, t, j).wait_recv()
                load(r2, c, t, j, 2).start()

            @pl.when(from_rx)
            def _():
                rx_p(c, t, j).wait_recv()

                @pl.when(relay)
                def _():
                    rx_f(c, t, j).start()

                load(rx, c, t, j, 2).start()

            buf = j % 2
            load(gx, c, t, j, buf).wait()
            at = 4 * c + t
            last = (j + 1) // nch
            nxt = at + last * (1 - again)
            nj = (j + 1) % nch

            @pl.when(nxt < 8)
            def _():
                load(gx, nxt // 4, nxt % 4, nj, 1 - buf).start()

            @pl.when(jnp.logical_not(keep_a))
            def _():
                project(buf, sel1, j)

            @pl.when(remote)
            def _():
                load(rx, c, t, j, 2).wait()

            rem = remote.astype(jnp.int32)
            project(buf * (1 - rem) + 2 * rem, sel2, j)

        step = 4

        def product(k):
            return lax.dot_general(AB[0, k], AB[1, k], (((1,), (1,)), ((), ())), preferred_element_type=F32)

        @pl.when(t == 0)
        def _():
            @pl.loop(0, ch // step)
            def _(k):
                for d in range(step):
                    O[p, k * step + d] = product(k * step + d)

        @pl.when(t > 0)
        def _():
            @pl.loop(0, ch // step)
            def _(k):
                for d in range(step):
                    O[p, k * step + d] += product(k * step + d)

    def put(c, b, p):
        src = st.at[b % 2]

        @pl.when(p == 0)
        def _():
            pltpu.make_async_copy(src, tile(ex, c, b), o_sem.at[b % 2]).start()

        @pl.when(p == 1)
        def _():
            pltpu.make_async_copy(src, tile(on, c, b), o_sem.at[b % 2]).start()

    def put_done(c, b, p):
        pltpu.make_async_copy(st.at[b % 2], tile(ex, c, b), o_sem.at[b % 2]).wait()

        @pl.when(p == 0)
        def _():
            t_c(c, b).start()

    def close(c, p):
        @pl.loop(0, n_b)
        def _(b):
            @pl.loop(0, per)
            def _(g):
                i0 = pl.multiple_of((b * per + g) * G8, G8)
                v = O[p, :, pl.ds(i0, G8), :]
                v = v - jnp.mean(v, axis=0, keepdims=True)
                var = jnp.mean(v * v, axis=0, keepdims=True)
                v = v * lax.rsqrt(var + 1e-5) * so[...]
                st[b % 2, g] = v.reshape(ch * G8, v.shape[2]).astype(BF16)

            put(c, b, p)

            @pl.when(b >= 1)
            def _():
                put_done(c, b - 1, p)

        put_done(c, n_b - 1, p)

    @pl.when(has_own)
    def _():
        load(gx, 0, 0, 0, 0).start()

        @pl.loop(0, 2)
        def _(c):
            @pl.loop(0, 4)
            def _(t):
                @pl.loop(0, 2)
                def _(p):
                    @pl.when((p == 1) | extra)
                    def _():
                        steps(c, t, p)

                        @pl.when(t == 3)
                        def _():
                            close(c, p)

    @pl.loop(0, 2)
    def _(c):
        @pl.when(end & jnp.logical_not(even))
        def _():
            @pl.loop(0, n_b)
            def _(b):
                t_c(c, b).wait_recv()

        @pl.when(extra)
        def _():
            @pl.loop(0, n_b)
            def _(b):
                t_c(c, b).wait_send()

        @pl.loop(0, nch)
        def _(j):
            p_in(c, j).wait_send()

            @pl.when(mid)
            def _():
                fwd(0, c, j).wait_send()

                @pl.when(even)
                def _():
                    p_out(c, j).wait_send()
                    fwd(1, c, j).wait_send()
                    fwd(2, c, j).wait_send()

            @pl.loop(0, 4)
            def _(t):
                @pl.when(owner)
                def _():
                    rx_c(c, t, j).wait_send()

                @pl.when(wide_owner)
                def _():
                    rx_p(c, t, j).wait_send()

                @pl.when(relay)
                def _():
                    rx_f(c, t, j).wait_send()

                @pl.when(r2_from)
                def _():
                    r2_c(c, t, j).wait_send()


def solution(mesh):
    nch = 4

    def device_fn(z_one, z_two, mask_one, mask_two, ln_in_scale, w_a, w_a_gate, w_b, w_b_gate, w_gate, w_out, ln_out_scale):
        n_i, n_k, ch = z_one.shape
        zt = [jnp.swapaxes(v, 1, 2) for v in (z_one, z_two)]
        s_in = jnp.broadcast_to(ln_in_scale.astype(F32)[:, None], (ch, n_k))
        s_out = jnp.broadcast_to(ln_out_scale.astype(F32)[:, None, None], (ch, G8, n_k))
        br = 16
        zspec = pl.BlockSpec((br, ch, n_k), lambda i: (i, 0, 0))
        mspec = pl.BlockSpec((br, n_k), lambda i: (i, 0))

        def fixed(*shape):
            return pl.BlockSpec(shape, lambda i: (0,) * len(shape))

        big = G8 * ch
        xm, w_ab, w_g, w_o = pl.pallas_call(
            norm_kernel,
            grid=(n_i // br,),
            in_specs=[zspec, zspec, mspec, mspec, fixed(ch, n_k)] + [fixed(ch, ch)] * 6,
            out_specs=(
                pl.BlockSpec((2, 1, br, ch, n_k), lambda i: (0, 0, i, 0, 0)),
                fixed(2, 2, big, big),
                fixed(big, big),
                fixed(big, big),
            ),
            out_shape=(
                jax.ShapeDtypeStruct((2, 4, n_i, ch, n_k), BF16),
                jax.ShapeDtypeStruct((2, 2, big, big), BF16),
                jax.ShapeDtypeStruct((big, big), BF16),
                jax.ShapeDtypeStruct((big, big), BF16),
            ),
            name="norm_in",
        )(zt[0], zt[1], mask_one, mask_two, s_in, w_a, w_a_gate, w_b, w_b_gate, w_gate, w_out)

        n_g = n_i // G8
        anyspec = pl.BlockSpec(memory_space=pl.ANY)
        vspec = pl.BlockSpec(memory_space=pltpu.VMEM)
        dma = pltpu.SemaphoreType.DMA
        cr = n_i // nch
        per = 2
        on, _, _, _, _ = pl.pallas_call(
            functools.partial(tri_kernel, nch, ch),
            out_shape=(
                jax.ShapeDtypeStruct((2, n_g, ch * G8, n_k), BF16),
                jax.ShapeDtypeStruct((2, 4, n_i, ch, n_k), BF16),
                jax.ShapeDtypeStruct((2, 4, n_i, ch, n_k), BF16),
                jax.ShapeDtypeStruct((2, 4, n_i, ch, n_k), BF16),
                jax.ShapeDtypeStruct((2, n_g, ch * G8, n_k), BF16),
            ),
            in_specs=[anyspec, vspec, vspec],
            out_specs=(anyspec,) * 5,
            input_output_aliases={0: 1},
            scratch_shapes=[
                pltpu.VMEM((2, ch, n_i, n_k), BF16),
                pltpu.VMEM((2, ch, n_i, n_k), F32),
                pltpu.VMEM((3, cr, ch, n_k), BF16),
                pltpu.VMEM((2, per, ch * G8, n_k), BF16),
                dma((2, 3, nch)),
                dma((2, 4, nch)),
                dma((2, 4, nch)),
                dma((2, n_g // per)),
                dma((2, nch)),
                dma((2, nch)),
                dma((2, 3, nch)),
                dma((2, 4, nch)),
                dma((2, 4, nch)),
                dma((2, 4, nch)),
                dma((2, n_g // per)),
                dma((3,)),
                dma((2,)),
            ],
            compiler_params=pltpu.CompilerParams(has_side_effects=True, vmem_limit_bytes=63 * 1024 * 1024),
            name="triangle",
        )(xm, w_ab, s_out)

        onspec = [pl.BlockSpec((1, br // G8, big, n_k), lambda i, crop=crop: (crop, i, 0, 0)) for crop in range(2)]
        outs = pl.pallas_call(
            finish_kernel,
            grid=(n_i // br,),
            in_specs=[zspec, zspec, *onspec, fixed(ch, n_k), fixed(big, big), fixed(big, big)],
            out_specs=(zspec, zspec),
            out_shape=(jax.ShapeDtypeStruct((n_i, ch, n_k), BF16),) * 2,
            name="finish",
        )(zt[0], zt[1], on, on, s_in, w_g, w_o)
        return tuple(jnp.swapaxes(out, 1, 2) for out in outs)

    pair_spec = P(("batch", "row"), "col", None)
    mask_spec = P(("batch", "row"), "col")
    rep = P()
    return jax.shard_map(
        device_fn,
        mesh=mesh,
        in_specs=(pair_spec, pair_spec, mask_spec, mask_spec) + (rep,) * 8,
        out_specs=(pair_spec, pair_spec),
        check_vma=False,
    )
```

```python
import functools

import jax
import jax.numpy as jnp
from jax import lax
from jax.experimental import pallas as pl
from jax.experimental.pallas import tpu as pltpu
from jax.sharding import PartitionSpec as P

MESH = pl.DeviceIdType.MESH
F32 = jnp.float32
BF16 = jnp.bfloat16
G8 = 8


def grow(w, first, count, rows_inner, cols_inner):
    k, m = w.shape
    i_r, i_m = (lax.broadcasted_iota(jnp.int32, (G8 * count, m), d) for d in (0, 1))
    i_k, i_c = (lax.broadcasted_iota(jnp.int32, (k, G8 * k), d) for d in (0, 1))
    pick_r = ((i_r // G8 if rows_inner else i_r % count) + first == i_m).astype(F32).astype(BF16)
    pick_c = ((i_c // G8 if cols_inner else i_c % k) == i_k).astype(F32).astype(BF16)
    big = lax.dot_general(pick_r, w, (((1,), (1,)), ((), ())), preferred_element_type=F32).astype(BF16)
    big = jnp.dot(big, pick_c, preferred_element_type=F32) * 0.5
    b_r, b_c = (lax.broadcasted_iota(jnp.int32, (G8 * count, G8 * k), d) for d in (0, 1))
    row_r = b_r % G8 if rows_inner else b_r // count
    row_c = b_c % G8 if cols_inner else b_c // k
    return jnp.where(row_r == row_c, big, 0.0).astype(BF16)


def layer_norm_row(zf, scale, keep):
    v = zf - jnp.mean(zf, axis=0, keepdims=True)
    rstd = lax.rsqrt(jnp.mean(v * v, axis=0, keepdims=True) + 1e-5)
    if keep is not None:
        rstd = rstd * keep
    return v * rstd * scale


def norm_kernel(z0, z1, m0, m1, s, wa, wag, wb, wbg, wg, wo, out, w_ab, w_g, w_o):
    @pl.when(pl.program_id(0) == 0)
    def _():
        ch = wa.shape[0]
        hc = ch // 2
        for side, ws in enumerate(((wa, wag), (wb, wbg))):
            for p in range(2):
                for kind in range(2):
                    part = slice(kind * hc * G8, (kind + 1) * hc * G8)
                    w_ab[side, p, part, :] = grow(ws[kind][...], p * hc, hc, True, False)
        w_g[...] = grow(wg[...], 0, ch, False, False)
        w_o[...] = grow(wo[...], 0, ch, False, True)

    scale = s[...]
    for crop, (z, m) in enumerate(((z0, m0), (z1, m1))):
        @pl.loop(0, z.shape[0] // G8)
        def _(g):
            i0 = pl.multiple_of(g * G8, G8)
            keep = m[pl.ds(i0, G8), :].astype(F32)
            for d in range(G8):
                x = layer_norm_row(z[i0 + d].astype(F32), scale, keep[d:d + 1])
                out[crop, 0, i0 + d] = x.astype(BF16)


def finish_kernel(z0, z1, on0, on1, s, wg, wo, out0, out1):
    scale = s[...]
    for z, on, out in ((z0, on0, out0), (z1, on1, out1)):
        ch, n_k = z.shape[1:]
        for g in range(z.shape[0] // G8):
            half = jnp.dot(wo[...], on[0, g], preferred_element_type=F32)
            for d in range(0, G8, 4):
                r = g * G8 + d
                x = jnp.concatenate(
                    [layer_norm_row(z[r + e].astype(F32), scale, None).astype(BF16) for e in range(4)], axis=0)
                gate = jnp.dot(wg[:4 * ch, :4 * ch], x, preferred_element_type=F32)
                upd = (1.0 + jnp.tanh(gate)) * half[d * ch:(d + 4) * ch]
                for e in range(4):
                    out[r + e] = (z[r + e].astype(F32) + upd[e * ch:(e + 1) * ch]).astype(BF16)


def tri_kernel(nch, ch, gx_in, w, so, on, gx, rx, r2, ex, AB, O, xb, st,
               g_sem, r_sem, r2_sem, t_sem, s_in, s_out, s_f, s_r1, s_r2, s_x, s_t, l_sem, o_sem):
    del gx_in
    z = lax.axis_index("col")
    r = lax.axis_index("row")
    h = z // 2
    zz = z + h * (3 - 2 * z)
    q = r + h * (3 - 2 * r)
    inner = z + 1 - 2 * h
    outer = 3 * h
    partner = r + 1 - 2 * (r % 2)
    cross = 2 - h
    mid = zz == 1
    end = zz == 0
    even = q % 2 == 0
    owner = q == zz
    wide_owner = mid & (q == 1)
    relay = mid & (q == 2)
    rx_here = (mid & (q != 1)) | (end & (q == 2))
    extra = mid & (q < 2)
    has_own = mid | even
    r2_from = mid & ((q == 0) | (q == 3))
    r2_row = (1 - (q // 3)) * partner + (q // 3) * 3 * h
    t_row = (1 - q) * (3 - 3 * h) + q * r
    n_i, n_k = gx.shape[2], gx.shape[4]
    cr = n_i // nch
    n_g = n_i // G8
    per = st.shape[1]
    n_b = n_g // per

    def rows(j):
        return pl.ds(pl.multiple_of(j * cr, cr), cr)

    def gs(c, t, j):
        return gx.at[c, t, rows(j)]

    def rs(c, t, j):
        return rx.at[c, t, rows(j)]

    def r2s(c, t, j):
        return r2.at[c, t, rows(j)]

    def cp(src, dst, ssem, rsem, col, row):
        return pltpu.make_async_remote_copy(src_ref=src, dst_ref=dst, send_sem=ssem, recv_sem=rsem,
                                            device_id={"col": col, "row": row}, device_id_type=MESH)

    def p_in(c, j):
        return cp(gs(c, 0, j), gs(c, 1 + zz, j), s_in.at[c, j], g_sem.at[c, zz, j], inner, r)

    def p_out(c, j):
        return cp(gs(c, 0, j), gs(c, 1, j), s_out.at[c, j], g_sem.at[c, 0, j], outer, r)

    def fwd(n, c, j):
        src, dst, col = ((1, 3, inner), (2, 2, outer), (3, 3, outer))[n]
        return cp(gs(c, src, j), gs(c, dst, j), s_f.at[c, n, j], g_sem.at[c, dst - 1, j], col, r)

    def wait_g(c, t, j):
        cp(gs(c, t, j), gs(c, t, j), s_in.at[c, j], g_sem.at[c, t - 1, j], z, r).wait_recv()

    def rx_p(c, t, j):
        return cp(gs(c, t, j), rs(c, t, j), s_r1.at[c, t, j], r_sem.at[c, t, j], z, partner)

    def rx_c(c, t, j):
        return cp(gs(c, t, j), rs(c, t, j), s_r2.at[c, t, j], r_sem.at[c, t, j], z, cross)

    def rx_f(c, t, j):
        return cp(rs(c, t, j), rs(c, t, j), s_r1.at[c, t, j], r_sem.at[c, t, j], z, partner)

    def r2_c(c, t, j):
        return cp(gs(c, t, j), r2s(c, t, j), s_x.at[c, t, j], r2_sem.at[c, t, j], z, r2_row)

    def tile(ref, c, b):
        return ref.at[c, pl.ds(pl.multiple_of(b * per, per), per)]

    def t_c(c, b):
        return cp(tile(ex, c, b), tile(on, c, b), s_t.at[c, b], t_sem.at[c, b], outer, t_row)

    def side_sends(c, t, j):
        @pl.when(owner)
        def _():
            rx_c(c, t, j).start()

        @pl.when(wide_owner)
        def _():
            rx_p(c, t, j).start()

        @pl.when(r2_from)
        def _():
            r2_c(c, t, j).start()

    @pl.loop(0, nch)
    def _(j):
        p_in(0, j).start()
        side_sends(0, 0, j)

        @pl.when(mid & even)
        def _():
            p_out(0, j).start()

    @pl.when(end)
    def _():
        @pl.loop(0, nch)
        def _(j):
            p_in(1, j).start()

    def comm_near(c, j):
        wait_g(c, 1, j)

        @pl.when(mid)
        def _():
            fwd(0, c, j).start()

        side_sends(c, 1, j)
        wait_g(c, 2, j)

        @pl.when(mid & even)
        def _():
            fwd(1, c, j).start()

        side_sends(c, 2, j)

    def comm_far(c, j):
        @pl.when((c == 0) & mid)
        def _():
            p_in(1, j).start()

        wait_g(c, 3, j)

        @pl.when(mid & even)
        def _():
            fwd(2, c, j).start()

        side_sends(c, 3, j)

        @pl.when(c == 0)
        def _():
            side_sends(1, 0, j)

            @pl.when(mid & even)
            def _():
                p_out(1, j).start()

    def comm(c, t, j):
        u = t * nch + j
        v = u % 8
        jj = v - 3 + (6 - v) // 4
        hit = (v == 2) | ((v >= 4) & (v <= 6))

        @pl.when(hit & (u < 8))
        def _():
            comm_near(c, jj)

        @pl.when(hit & (u >= 8))
        def _():
            comm_far(c, jj)

    half = w.shape[2] // 2

    def project(buf, sel, j):
        @pl.loop(0, cr // 16)
        def _(s):
            xs = xb[buf, pl.ds(pl.multiple_of(s * 16, 16), 16)]
            x0 = xs[:G8].reshape(G8 * ch, n_k)
            x1 = xs[G8:].reshape(G8 * ch, n_k)
            i0 = pl.multiple_of(j * cr + s * 16, 16)
            nc = half // G8
            for p in range(w.shape[1]):
                parts = []
                for xg in (x0, x1):
                    res = jnp.dot(w[sel, p], xg, preferred_element_type=F32)
                    val = res[:half] * (1.0 + jnp.tanh(res[half:]))
                    parts.append(val.reshape(nc, G8, n_k))
                AB[sel, p * nc:(p + 1) * nc, pl.ds(i0, 16), :] = jnp.concatenate(parts, axis=1).astype(BF16)

    def load(ref, c, t, j, buf):
        return pltpu.make_async_copy(ref.at[c, t, rows(j)], xb.at[buf], l_sem.at[buf])

    def steps(c, t, p):
        first_b = (p == 0) & (q == 0)
        from_r2 = p == 0
        from_rx = (p == 1) & rx_here
        remote = from_r2 | from_rx
        keep_a = (p == 1) & extra & (q == 1)
        sel1 = first_b.astype(jnp.int32)
        sel2 = 1 - sel1
        again = ((p == 0) & extra).astype(jnp.int32)

        @pl.loop(0, nch)
        def _(j):
            @pl.when((p == 0) | jnp.logical_not(extra))
            def _():
                comm(c, t, j)

            @pl.when(from_r2)
            def _():
                r2_c(c, t, j).wait_recv()
                load(r2, c, t, j, 2).start()

            @pl.when(from_rx)
            def _():
                rx_p(c, t, j).wait_recv()

                @pl.when(relay)
                def _():
                    rx_f(c, t, j).start()

                load(rx, c, t, j, 2).start()

            buf = j % 2
            load(gx, c, t, j, buf).wait()
            at = 4 * c + t
            last = (j + 1) // nch
            nxt = at + last * (1 - again)
            nj = (j + 1) % nch

            @pl.when(nxt < 8)
            def _():
                load(gx, nxt // 4, nxt % 4, nj, 1 - buf).start()

            @pl.when(jnp.logical_not(keep_a))
            def _():
                project(buf, sel1, j)

            @pl.when(remote)
            def _():
                load(rx, c, t, j, 2).wait()

            rem = remote.astype(jnp.int32)
            project(buf * (1 - rem) + 2 * rem, sel2, j)

        step = 4

        def product(k):
            return lax.dot_general(AB[0, k], AB[1, k], (((1,), (1,)), ((), ())), preferred_element_type=F32)

        @pl.when(t == 0)
        def _():
            @pl.loop(0, ch // step)
            def _(k):
                for d in range(step):
                    O[p, k * step + d] = product(k * step + d)

        @pl.when(t > 0)
        def _():
            @pl.loop(0, ch // step)
            def _(k):
                for d in range(step):
                    O[p, k * step + d] += product(k * step + d)

    def put(c, b, p):
        src = st.at[b % 2]

        @pl.when(p == 0)
        def _():
            pltpu.make_async_copy(src, tile(ex, c, b), o_sem.at[b % 2]).start()

        @pl.when(p == 1)
        def _():
            pltpu.make_async_copy(src, tile(on, c, b), o_sem.at[b % 2]).start()

    def put_done(c, b, p):
        pltpu.make_async_copy(st.at[b % 2], tile(ex, c, b), o_sem.at[b % 2]).wait()

        @pl.when(p == 0)
        def _():
            t_c(c, b).start()

    def close(c, p):
        @pl.loop(0, n_b)
        def _(b):
            @pl.loop(0, per)
            def _(g):
                i0 = pl.multiple_of((b * per + g) * G8, G8)
                v = O[p, :, pl.ds(i0, G8), :]
                v = v - jnp.mean(v, axis=0, keepdims=True)
                var = jnp.mean(v * v, axis=0, keepdims=True)
                v = v * lax.rsqrt(var + 1e-5) * so[...]
                st[b % 2, g] = v.reshape(ch * G8, v.shape[2]).astype(BF16)

            put(c, b, p)

            @pl.when(b >= 1)
            def _():
                put_done(c, b - 1, p)

        put_done(c, n_b - 1, p)

    @pl.when(has_own)
    def _():
        load(gx, 0, 0, 0, 0).start()

        @pl.loop(0, 2)
        def _(c):
            @pl.loop(0, 4)
            def _(t):
                @pl.loop(0, 2)
                def _(p):
                    @pl.when((p == 1) | extra)
                    def _():
                        steps(c, t, p)

                        @pl.when(t == 3)
                        def _():
                            close(c, p)

    @pl.loop(0, 2)
    def _(c):
        @pl.when(end & jnp.logical_not(even))
        def _():
            @pl.loop(0, n_b)
            def _(b):
                t_c(c, b).wait_recv()

        @pl.when(extra)
        def _():
            @pl.loop(0, n_b)
            def _(b):
                t_c(c, b).wait_send()

        @pl.loop(0, nch)
        def _(j):
            p_in(c, j).wait_send()

            @pl.when(mid)
            def _():
                fwd(0, c, j).wait_send()

                @pl.when(even)
                def _():
                    p_out(c, j).wait_send()
                    fwd(1, c, j).wait_send()
                    fwd(2, c, j).wait_send()

            @pl.loop(0, 4)
            def _(t):
                @pl.when(owner)
                def _():
                    rx_c(c, t, j).wait_send()

                @pl.when(wide_owner)
                def _():
                    rx_p(c, t, j).wait_send()

                @pl.when(relay)
                def _():
                    rx_f(c, t, j).wait_send()

                @pl.when(r2_from)
                def _():
                    r2_c(c, t, j).wait_send()


def solution(mesh):
    nch = 4

    def device_fn(z_one, z_two, mask_one, mask_two, ln_in_scale, w_a, w_a_gate, w_b, w_b_gate, w_gate, w_out, ln_out_scale):
        n_i, n_k, ch = z_one.shape
        zt = [jnp.swapaxes(v, 1, 2) for v in (z_one, z_two)]
        s_in = jnp.broadcast_to(ln_in_scale.astype(F32)[:, None], (ch, n_k))
        s_out = jnp.broadcast_to(ln_out_scale.astype(F32)[:, None, None], (ch, G8, n_k))
        br = 16
        zspec = pl.BlockSpec((br, ch, n_k), lambda i: (i, 0, 0))
        mspec = pl.BlockSpec((br, n_k), lambda i: (i, 0))

        def fixed(*shape):
            return pl.BlockSpec(shape, lambda i: (0,) * len(shape))

        big = G8 * ch
        xm, w_ab, w_g, w_o = pl.pallas_call(
            norm_kernel,
            grid=(n_i // br,),
            in_specs=[zspec, zspec, mspec, mspec, fixed(ch, n_k)] + [fixed(ch, ch)] * 6,
            out_specs=(
                pl.BlockSpec((2, 1, br, ch, n_k), lambda i: (0, 0, i, 0, 0)),
                fixed(2, 2, big, big),
                fixed(big, big),
                fixed(big, big),
            ),
            out_shape=(
                jax.ShapeDtypeStruct((2, 4, n_i, ch, n_k), BF16),
                jax.ShapeDtypeStruct((2, 2, big, big), BF16),
                jax.ShapeDtypeStruct((big, big), BF16),
                jax.ShapeDtypeStruct((big, big), BF16),
            ),
            name="norm_in",
        )(zt[0], zt[1], mask_one, mask_two, s_in, w_a, w_a_gate, w_b, w_b_gate, w_gate, w_out)

        n_g = n_i // G8
        anyspec = pl.BlockSpec(memory_space=pl.ANY)
        vspec = pl.BlockSpec(memory_space=pltpu.VMEM)
        dma = pltpu.SemaphoreType.DMA
        cr = n_i // nch
        per = 2
        on, _, _, _, _ = pl.pallas_call(
            functools.partial(tri_kernel, nch, ch),
            out_shape=(
                jax.ShapeDtypeStruct((2, n_g, ch * G8, n_k), BF16),
                jax.ShapeDtypeStruct((2, 4, n_i, ch, n_k), BF16),
                jax.ShapeDtypeStruct((2, 4, n_i, ch, n_k), BF16),
                jax.ShapeDtypeStruct((2, 4, n_i, ch, n_k), BF16),
                jax.ShapeDtypeStruct((2, n_g, ch * G8, n_k), BF16),
            ),
            in_specs=[anyspec, vspec, vspec],
            out_specs=(anyspec,) * 5,
            input_output_aliases={0: 1},
            scratch_shapes=[
                pltpu.VMEM((2, ch, n_i, n_k), BF16),
                pltpu.VMEM((2, ch, n_i, n_k), F32),
                pltpu.VMEM((3, cr, ch, n_k), BF16),
                pltpu.VMEM((2, per, ch * G8, n_k), BF16),
                dma((2, 3, nch)),
                dma((2, 4, nch)),
                dma((2, 4, nch)),
                dma((2, n_g // per)),
                dma((2, nch)),
                dma((2, nch)),
                dma((2, 3, nch)),
                dma((2, 4, nch)),
                dma((2, 4, nch)),
                dma((2, 4, nch)),
                dma((2, n_g // per)),
                dma((3,)),
                dma((2,)),
            ],
            compiler_params=pltpu.CompilerParams(has_side_effects=True, vmem_limit_bytes=63 * 1024 * 1024),
            name="triangle",
        )(xm, w_ab, s_out)

        onspec = [pl.BlockSpec((1, br // G8, big, n_k), lambda i, crop=crop: (crop, i, 0, 0)) for crop in range(2)]
        outs = pl.pallas_call(
            finish_kernel,
            grid=(n_i // br,),
            in_specs=[zspec, zspec, *onspec, fixed(ch, n_k), fixed(big, big), fixed(big, big)],
            out_specs=(zspec, zspec),
            out_shape=(jax.ShapeDtypeStruct((n_i, ch, n_k), BF16),) * 2,
            name="finish",
        )(zt[0], zt[1], on, on, s_in, w_g, w_o)
        return tuple(jnp.swapaxes(out, 1, 2) for out in outs)

    pair_spec = P(("batch", "row"), "col", None)
    mask_spec = P(("batch", "row"), "col")
    rep = P()
    return jax.shard_map(
        device_fn,
        mesh=mesh,
        in_specs=(pair_spec, pair_spec, mask_spec, mask_spec) + (rep,) * 8,
        out_specs=(pair_spec, pair_spec),
        check_vma=False,
    )
```
